32 devices in a mesh: dp: 16 (over z, y, core), mp: 2 (over x).
Axes of the slice: x: 2, y: 2, z: 4, core: 2. Of those that a mesh axis runs over, the one named last changes fastest.
Arguments:
- x_cache: bfloat16 [2, 16, 197, 1024], P(None, 'dp'), may hold values from -6 to 6
- w_in: bfloat16 [2, 1024, 2048], P(None, None, 'mp'), may hold values from -0.1875 to 0.1875
- w_out: bfloat16 [2, 2048, 1024], P(None, 'mp'), may hold values from -0.125 to 0.125
- top_grad: bfloat16 [16, 197, 1024], P('dp')
- layer_mask: int32 [16, 2], P('dp'), may hold values from 0 to 1, as said below
- target: int32 [1], replicated, may hold values from 2 to 13
Outputs:
- grad_in: float32 [2, 1024, 2048], P(None, 'dp', 'mp')
- grad_out: float32 [2, 2048, 1024], P(None, 'mp', 'dp')
- threshold: float32 [1], replicated
The draws below stay inside these ranges and needn't reach their ends.
Inputs may be any that keep to these rules, and one draw needn't show every extreme that they name: `layer_mask`: every example has at least one block with mask 1.
All inputs are finite; a program needn't handle non-finite values.
Results may differ from the reference program's by a relative error of at most 0.0013.
Values sent between devices are 32-bit elements; how exact they have to be, the bound alone decides.
No kernel may reach another device: no remote copies, remote signals or barrier semaphores. Data moves between devices by JAX's collectives and lax.ppermute only.
A program may use at most 64 MiB of HBM per device.

```python
import jax
import jax.numpy as jnp
from jax import lax

D = 1024
FF = 2048
TOK = 197
LAYERS = 2
EXAMPLES = 16


def draw_x_cache(key, part):
    key_noise = jax.random.fold_in(key, 31)
    key_own = jax.random.fold_in(key, 32)
    key_share = jax.random.fold_in(key, 33)
    share = jax.random.uniform(key_share, (LAYERS, EXAMPLES, 1, 1), jnp.float32, 0.4, 0.8)
    rest = jnp.sqrt(1.0 - share * share)
    own = jax.random.normal(key_own, (LAYERS, EXAMPLES, 1, D), jnp.float32)
    noise = jax.random.normal(key_noise, (LAYERS, EXAMPLES, TOK, D), jnp.float32)
    values = rest * noise + share * own
    return jnp.clip(values, -6.0, 6.0).astype(jnp.bfloat16)


def draw_top_grad(key, part):
    key_noise = jax.random.fold_in(key, 11)
    key_jitter = jax.random.fold_in(key, 12)
    key_own = jax.random.fold_in(key, 14)
    key_share = jax.random.fold_in(key, 15)
    position = jnp.arange(EXAMPLES, dtype=jnp.float32) / max(EXAMPLES - 1, 1)
    share = jax.random.uniform(key_share, (EXAMPLES, 1, 1), jnp.float32, 0.45, 0.85)
    rest = jnp.sqrt(1.0 - share * share)
    own = jax.random.normal(key_own, (EXAMPLES, 1, D), jnp.float32)
    jitter = jnp.exp(jax.random.uniform(key_jitter, (EXAMPLES,), jnp.float32, 0.0, 1.386294))
    noise = jax.random.normal(key_noise, (EXAMPLES, TOK, D), jnp.float32)
    values = rest * noise + share * own
    scales = jnp.exp(position * 1.098612) * jitter
    return (values * scales[:, None, None]).astype(jnp.bfloat16)


def draw_layer_mask(key, part):
    key_levels = jax.random.fold_in(key, 21)
    key_forced = jax.random.fold_in(key, 22)
    levels = jax.random.randint(key_levels, (EXAMPLES, LAYERS), 0, 4)
    active = (levels > 0).astype(jnp.int32)
    forced = jax.random.randint(key_forced, (EXAMPLES,), 0, LAYERS)
    chosen = (jnp.arange(LAYERS)[None, :] == forced[:, None]).astype(jnp.int32)
    return jnp.maximum(active, chosen)


def shard_levels(rng, extent, cuts, smallest, largest):
    factor_of, own = 1.0, jax.random.fold_in(rng, 6)
    for axis_at, shards_of in cuts:
        draws = jnp.exp(jax.random.uniform(jax.random.fold_in(own, axis_at), (shards_of,), jnp.float32, smallest / len(cuts), largest / len(cuts)))
        factor_of = factor_of * jnp.repeat(draws, extent[axis_at] // shards_of).reshape([-1 if axis == axis_at else 1 for axis in range(len(extent))])
    return factor_of


def normal_values(key, extent, width, limit, shards=(), kind=jnp.bfloat16):
    drawn = jax.random.normal(key, extent, jnp.float32) * width
    if len(shards) > 0:
        drawn = shard_levels(key, extent, shards, -0.22, 0.18) * drawn
    return jnp.clip(drawn, min=-limit, max=limit).astype(kind)


def setup_inputs(seed: int = 0) -> dict:
    key_list = jax.random.split(jax.random.key(seed), 7)
    return {
        "x_cache": draw_x_cache(jax.random.fold_in(key_list[6], 71), 0),
        "w_in": normal_values(key_list[1], (LAYERS, D, FF), D ** -0.5, 0.1875, ((2, 2),)),
        "w_out": normal_values(key_list[2], (LAYERS, FF, D), FF ** -0.5, 0.125, ((1, 2),)),
        "top_grad": draw_top_grad(jax.random.fold_in(key_list[6], 71), 0),
        "layer_mask": draw_layer_mask(jax.random.fold_in(key_list[6], 71), 0),
        "target": jax.random.randint(key_list[5], (1,), EXAMPLES // 8, 7 * EXAMPLES // 8).astype(jnp.int32),
    }


def normalize(values):
    average = lax.optimization_barrier(jnp.mean(values, -1, keepdims=True))
    centered = values - average
    spread = lax.optimization_barrier(jnp.mean(centered * centered, -1, keepdims=True))
    return centered * lax.rsqrt(spread + 1e-06)

def gelu_slope(preact):
    return 0.5 * (1.0 + lax.erf(preact * 0.7071067811865476)) + preact * jnp.exp(-0.5 * preact * preact) * 0.3989422804014327

def gram_matrix(values):
    wide = values.astype(jnp.float32)
    return jnp.einsum('etd,esd->ets', wide, wide)

def reference(x_cache, w_in, w_out, top_grad, layer_mask, target):
    examples = x_cache.shape[1]
    tokens = x_cache.shape[2]
    model_width = x_cache.shape[3]
    cotangent = top_grad.astype(jnp.float32)
    squares = jnp.zeros((examples,), jnp.float32)
    stored = []
    for depth in range(LAYERS - 1, -1, -1):
        inputs = x_cache[depth].astype(jnp.float32)
        normed = normalize(inputs).astype(jnp.bfloat16)
        flat_in = normed.reshape(-1, model_width)
        preact = jnp.dot(flat_in, w_in[depth], preferred_element_type=jnp.float32)
        hidden = jax.nn.gelu(preact, approximate=False).astype(jnp.bfloat16)
        keeper = layer_mask[:, depth].astype(jnp.float32)[:, None, None]
        outer_grad = (keeper * cotangent).astype(jnp.bfloat16)
        backed = jnp.dot(outer_grad.reshape(-1, model_width), w_out[depth].T, preferred_element_type=jnp.float32)
        inner_grad = (backed * gelu_slope(preact)).astype(jnp.bfloat16)
        inner3 = inner_grad.reshape(examples, tokens, -1)
        hidden3 = hidden.reshape(examples, tokens, -1)
        squares = squares + lax.optimization_barrier(jnp.sum(gram_matrix(normed) * gram_matrix(inner3), (1, 2)))
        squares = squares + lax.optimization_barrier(jnp.sum(gram_matrix(hidden3) * gram_matrix(outer_grad), (1, 2)))
        if depth > 0:
            summed = jnp.dot(inner_grad, w_in[depth].T, preferred_element_type=jnp.float32)
            summed = summed.reshape(examples, tokens, model_width)
            unused, pullback = jax.vjp(normalize, inputs)
            cotangent = cotangent + keeper * pullback(summed)[0]
        stored.append((flat_in, hidden, outer_grad.reshape(-1, model_width), inner3))
    stored = stored[::-1]
    norms = jnp.sqrt(squares)
    ordered = jnp.sort(norms)
    threshold = lax.dynamic_index_in_dim(ordered, (examples - 1 - target[0]).astype(jnp.int32), 0, keepdims=False)
    factor = jnp.minimum(1.0, threshold / norms) / examples
    grads_in = []
    grads_out = []
    for depth in range(LAYERS):
        flat_in, hidden, outer_flat, inner3 = stored[depth]
        scaled_inner = (factor[:, None, None] * inner3.astype(jnp.float32)).astype(jnp.bfloat16).reshape(examples * tokens, -1)
        scaled_outer = (jnp.repeat(factor, tokens)[:, None] * outer_flat.astype(jnp.float32)).astype(jnp.bfloat16)
        grads_in.append(jnp.dot(flat_in.T, scaled_inner, preferred_element_type=jnp.float32))
        grads_out.append(jnp.dot(hidden.T, scaled_outer, preferred_element_type=jnp.float32))
    return (jnp.stack(grads_in), jnp.stack(grads_out), threshold[None])
```

```python
import functools

import jax
import jax.numpy as jnp
from jax import lax
from jax.experimental import pallas as pl
from jax.experimental.pallas import tpu as pltpu
from jax.sharding import PartitionSpec as P


F32 = jnp.float32
BF16 = jnp.bfloat16
VMEM = pl.BlockSpec(memory_space=pltpu.VMEM)
SMEM = pl.BlockSpec(memory_space=pltpu.SMEM)


def call(body, out_shape, args, specs, flops, scratch=(), out_specs=None):
    return pl.pallas_call(
        body,
        out_shape=out_shape,
        in_specs=specs,
        out_specs=out_specs if out_specs is not None else jax.tree.map(lambda _: VMEM, out_shape),
        scratch_shapes=list(scratch),
        compiler_params=pltpu.CompilerParams(vmem_limit_bytes=56 * 1024 * 1024),
        cost_estimate=pl.CostEstimate(flops=flops, bytes_accessed=8 << 20, transcendentals=0),
    )(*args)


def matmul(left, right):
    return jnp.dot(left, right, preferred_element_type=F32)


def matmul_t(left, right):
    return lax.dot_general(left, right, (((1,), (1,)), ((), ())), preferred_element_type=F32)


def center(values):
    average = jnp.mean(values, -1, keepdims=True)
    centered = values - average
    spread = jnp.mean(centered * centered, -1, keepdims=True)
    inverse = lax.rsqrt(spread + 1e-06)
    return centered * inverse, inverse


def gelu_parts(preact):
    half_cdf = 0.5 * (1.0 + lax.erf(preact * 0.7071067811865476))
    slope = half_cdf + preact * jnp.exp(-0.5 * preact * preact) * 0.3989422804014327
    return preact * half_cdf, slope


def place():
    index = lax.axis_index("dp")
    core = lax.rem(index, 2)
    side = lax.rem(index // 2, 2)
    return index, core, side


def put_transposed(scratch, values, wide):
    pad = wide - values.shape[0]
    if pad:
        values = jnp.concatenate([values, jnp.zeros((pad, values.shape[1]), F32)], 0)
    scratch[...] = values.T


def pick_rows(scratch, target, rows, core, sides, own_side):
    blocks = target.shape[0] // rows
    for block in range(blocks):
        at = (2 * block + own_side) if sides else block
        start = pl.multiple_of((2 * at + core) * rows, rows)
        target[block * rows : (block + 1) * rows, :] = scratch[pl.ds(start, rows), :]


def layer_body(rows, with_back, x_ref, cot_ref, win_ref, wout_ref, ih_ref, keep_ref, send_ref, *rest):
    wide = keep_ref.shape[2]
    if with_back:
        back_ref, turned = rest
    else:
        (turned,) = rest
    unused, core, side = place()
    normed = center(x_ref[...])[0].astype(BF16)
    outer = cot_ref[...].astype(BF16)
    preact = matmul(normed, win_ref[...])
    hidden, slope = gelu_parts(preact)
    ih_ref[1] = hidden.astype(BF16).astype(F32)
    inner = (matmul_t(outer, wout_ref[...]) * slope).astype(BF16)
    ih_ref[0] = inner.astype(F32)
    if with_back:
        back_ref[...] = matmul_t(inner, win_ref[...])
    for at, values in ((0, normed), (1, outer)):
        put_transposed(turned, values.astype(F32), wide)
        pick_rows(turned, keep_ref.at[at], rows, core, True, side)
        pick_rows(turned, send_ref.at[at], rows, 1 - core, True, side)


def early_body(
    rows, x1_ref, cot_ref, ih1_ref, x0_ref, win_ref, hid_ref, slope_ref, keep_ref, send_ref, gram_ref, sq_ref, turned
):
    wide = keep_ref.shape[1]
    unused, core, side = place()
    normed = center(x0_ref[...].astype(F32))[0].astype(BF16)
    preact = matmul(normed, win_ref[...])
    hidden, slope = gelu_parts(preact)
    hidden = hidden.astype(BF16)
    hid_ref[...] = hidden.astype(F32)
    slope_ref[...] = slope
    put_transposed(turned, normed.astype(F32), wide)
    pick_rows(turned, keep_ref, rows, core, False, side)
    pick_rows(turned, send_ref, rows, 1 - core, False, side)
    gram_ref[0] = matmul_t(normed, normed)
    gram_ref[1] = matmul_t(hidden, hidden)
    upper = center(x1_ref[...])[0].astype(BF16)
    outer = cot_ref[...].astype(BF16)
    inner1 = ih1_ref[0].astype(BF16)
    hidden1 = ih1_ref[1].astype(BF16)
    total = matmul_t(upper, upper) * matmul_t(inner1, inner1)
    total = total + matmul_t(hidden1, hidden1) * matmul_t(outer, outer)
    sq_ref[...] = jnp.full(sq_ref.shape, jnp.sum(total), F32)


def late_body(
    rows, mask_ref, x1_ref, tg_ref, own_ref, recv_ref, slope_ref, gram_ref, sq1_ref, wout_ref,
    inner_ref, keep_ref, send_ref, sq_ref, turned,
):
    wide = keep_ref.shape[1]
    unused, core, side = place()
    mask0 = mask_ref[0, 0].astype(F32)
    mask1 = mask_ref[0, 1].astype(F32)
    normed, inverse = center(x1_ref[...])
    back = own_ref[...] + recv_ref[...]
    shift = jnp.mean(back, -1, keepdims=True)
    lean = jnp.mean(back * normed, -1, keepdims=True)
    pulled = inverse * (back - shift - normed * lean)
    outer = (mask0 * (tg_ref[...].astype(F32) + mask1 * pulled)).astype(BF16)
    inner = (matmul_t(outer, wout_ref[...]) * slope_ref[...]).astype(BF16)
    inner_ref[...] = inner.astype(F32)
    total = gram_ref[0] * matmul_t(inner, inner) + gram_ref[1] * matmul_t(outer, outer)
    sq_ref[...] = sq1_ref[...] + jnp.full(sq_ref.shape, jnp.sum(total), F32)
    put_transposed(turned, outer.astype(F32), wide)
    pick_rows(turned, keep_ref, rows, core, False, side)
    pick_rows(turned, send_ref, rows, 1 - core, False, side)


def norm_body(target_ref, sq_ref, factor_ref, threshold_ref):
    count, lanes = factor_ref.shape
    total = sq_ref[0:count, :]
    for at in range(1, sq_ref.shape[0] // count):
        total = total + sq_ref[at * count : (at + 1) * count, :]
    norm = jnp.sqrt(total)
    square = norm
    if count < lanes:
        square = jnp.concatenate([norm, jnp.zeros((lanes - count, lanes), F32)], 0)
    other = square.T[0:count, :]
    valid = lax.broadcasted_iota(jnp.int32, (count, lanes), 1) < count
    above = jnp.sum(jnp.where(valid & (other > norm), 1.0, 0.0), -1, keepdims=True)
    reach = jnp.sum(jnp.where(valid & (other >= norm), 1.0, 0.0), -1, keepdims=True)
    wanted = target_ref[0].astype(F32)
    hit = (above <= wanted) & (reach > wanted)
    threshold = jnp.max(jnp.where(hit, norm[:, 0:1], -1.0))
    factor_ref[...] = jnp.minimum(1.0, threshold / norm) / count
    threshold_ref[...] = jnp.full(threshold_ref.shape, threshold, F32)


def stack_scaled(scratch, values, factor, at, wide):
    pad = wide - values.shape[0]
    if pad:
        values = jnp.concatenate([values, jnp.zeros((pad, values.shape[1]), F32)], 0)
    if factor is not None:
        values = values * factor
    scratch[at * wide : (at + 1) * wide, :] = values.astype(BF16)


def lower_body(
    rows, factor_ref, i_ref, ip_ref, h_ref, hp_ref, nk_ref, np_ref, ok_ref, op_ref,
    send_ref, keep_ref, right, left,
):
    index, core, side = place()
    wide = nk_ref.shape[1]
    groups = keep_ref.shape[1]
    mine = factor_ref[index, 0]
    theirs = factor_ref[index + 1 - 2 * core, 0]
    for mat, first, second, t_own, t_other in (
        (0, i_ref, ip_ref, nk_ref, np_ref),
        (1, h_ref, hp_ref, ok_ref, op_ref),
    ):
        scale_right = mat == 0
        stack_scaled(right, first[...], mine if scale_right else None, 0, wide)
        stack_scaled(right, second[...], theirs if scale_right else None, 1, wide)
        for out_ref, chosen in ((send_ref, 1 - side), (keep_ref, side)):
            for at, source, factor in ((0, t_own, mine), (1, t_other, theirs)):
                for group in range(groups):
                    start = pl.multiple_of((2 * group + chosen) * rows, rows)
                    part = source[pl.ds(start, rows), :]
                    if not scale_right:
                        part = part * factor
                    left[group * rows : (group + 1) * rows, at * wide : (at + 1) * wide] = part.astype(BF16)
            out_ref[mat] = matmul(left[...], right[...]).reshape(groups, rows, -1)


def upper_body(
    rows, factor_ref, ih_ref, ihp_ref, ihy_ref, ihyp_ref, k_ref, p_ref, ky_ref, yp_ref,
    keep_ref, right, left,
):
    index, core, side = place()
    wide = k_ref.shape[2]
    groups = keep_ref.shape[1]
    partner = index + 1 - 2 * core
    across = index + 2 - 4 * side
    factors = [factor_ref[at, 0] for at in (index, partner, across, across + 1 - 2 * core)]
    for mat in range(2):
        for at, (source, turned) in enumerate(((ih_ref, k_ref), (ihp_ref, p_ref), (ihy_ref, ky_ref), (ihyp_ref, yp_ref))):
            stack_scaled(right, source[mat], factors[at] if mat == 0 else None, at, wide)
            part = turned[mat]
            if mat == 1:
                part = part * factors[at]
            left[:, at * wide : (at + 1) * wide] = part.astype(BF16)
        keep_ref[mat] = matmul(left[...], right[...]).reshape(groups, rows, -1)


def local(ways, mp, x_cache, w_in, w_out, top_grad, layer_mask, target):
    layers, examples, tokens, width = x_cache.shape
    hidden = w_in.shape[2]
    assert examples == 1 and layers == 2 and ways % 4 == 0
    groups = ways // 4
    rows = width // ways
    padded = -(-tokens // 16) * 16
    wide = -(-tokens // 128) * 128
    half = width // 2
    index = lax.axis_index("dp")
    level = index // 4

    def swap(step):
        return [(at, at ^ step) for at in range(ways)]

    def over_core(values):
        return lax.ppermute(values, "dp", swap(1))

    def over_side(values):
        return lax.ppermute(values, "dp", swap(2))

    def shape(*extent):
        return jax.ShapeDtypeStruct(extent, F32)

    def widen(values, kind):
        return jnp.pad(values.astype(kind), ((0, padded - tokens), (0, 0)))

    mask1 = layer_mask[0, 1].astype(F32)
    x1 = widen(x_cache[1, 0], F32)
    cot = widen(mask1 * top_grad[0].astype(F32), F32)
    plain = widen(top_grad[0], BF16)
    x0 = widen(x_cache[0, 0], BF16)
    x1y = over_side(x1)
    coty = over_side(cot)

    unit = 2 * padded * width * hidden
    turned = pltpu.VMEM((width, wide), F32)
    layer_out = (shape(2, padded, hidden), shape(2, half // 2, wide), shape(2, half // 2, wide))
    ih1, t1, t1s, back = call(
        functools.partial(layer_body, rows, True),
        layer_out + (shape(padded, width),),
        (x1, cot, w_in[1], w_out[1]),
        [VMEM] * 4,
        3 * unit,
        [turned],
    )
    moved = None
    for step in range(1, mp):
        part = lax.ppermute(back, "mp", [(at, (at + step) % mp) for at in range(mp)])
        moved = part if moved is None else moved + part
    ih1p, t1p = over_core(ih1), over_core(t1s)
    h0, slope, tn0, tn0s, gram, sq1 = call(
        functools.partial(early_body, rows),
        (
            shape(padded, hidden), shape(padded, hidden), shape(half, wide), shape(half, wide),
            shape(2, padded, padded), shape(8, 128),
        ),
        (x1, cot, ih1, x0, w_in[0]),
        [VMEM] * 5,
        2 * unit,
        [turned],
    )
    h0p, tn0p = over_core(h0), over_core(tn0s)
    i0, to0, to0s, sq = call(
        functools.partial(late_body, rows),
        (shape(padded, hidden), shape(half, wide), shape(half, wide), shape(8, 128)),
        (layer_mask, x1, plain, back, moved, slope, gram, sq1, w_out[0]),
        [SMEM] + [VMEM] * 8,
        2 * unit,
        [turned],
    )
    spread = jnp.broadcast_to(sq[0:1], (ways * mp, 128))
    squares = lax.all_to_all(spread, ("mp", "dp"), 0, 0, tiled=True)
    i0p, to0p = over_core(i0), over_core(to0s)
    ihy, ty, tys = call(
        functools.partial(layer_body, rows, False),
        layer_out,
        (x1y, coty, w_in[1], w_out[1]),
        [VMEM] * 4,
        2 * unit,
        [turned],
    )
    ihyp, typ = over_core(ihy), over_core(tys)
    factor, threshold = call(norm_body, (shape(ways, 128), shape(8, 128)), (target, squares), [SMEM, VMEM], 1 << 16)

    tile = shape(2, groups, rows, hidden)
    send0, keep0 = call(
        functools.partial(lower_body, rows),
        (tile, tile),
        (factor, i0, i0p, h0, h0p, tn0, tn0p, to0, to0p),
        [SMEM] + [VMEM] * 8,
        2 * unit,
        [pltpu.VMEM((2 * wide, hidden), BF16), pltpu.VMEM((half // 2, 2 * wide), BF16)],
    )
    keep1 = call(
        functools.partial(upper_body, rows),
        tile,
        (factor, ih1, ih1p, ihy, ihyp, t1, t1p, ty, typ),
        [SMEM] + [VMEM] * 8,
        2 * unit,
        [pltpu.VMEM((4 * wide, hidden), BF16), pltpu.VMEM((half // 2, 4 * wide), BF16)],
    )

    def line(parts):
        def slice_at(at):
            at = jnp.clip(at, 0, groups - 1)
            return sum(lax.dynamic_index_in_dim(part, at, 0, keepdims=False) for part in parts)

        up, down = None, None
        for step in range(1, groups):
            rising = slice_at(level + groups - step)
            falling = slice_at(level - groups + step)
            rising = rising if up is None else rising + up
            falling = falling if down is None else falling + down
            up_pairs, down_pairs = [], []
            for at in range(ways):
                layer = at // 4
                if layer <= step - 1 and layer + 1 < groups:
                    up_pairs.append((at, at + 4))
                if groups - 1 - layer <= step - 1 and layer > 0:
                    down_pairs.append((at, at - 4))
            up = lax.ppermute(rising, "dp", up_pairs)
            down = lax.ppermute(falling, "dp", down_pairs)
        return slice_at(level) + up + down

    moved0 = [over_side(send0[mat]) for mat in range(2)]
    final1 = [line([keep1[mat]]) for mat in range(2)]
    final0 = [line([keep0[mat], moved0[mat]]) for mat in range(2)]
    grad_in = jnp.stack([final0[0], final1[0]])
    grad_out = jnp.stack([final0[1].T, final1[1].T])
    return grad_in, grad_out, threshold[0, 0:1]


def solution(mesh):
    ways, mp = mesh.shape["dp"], mesh.shape["mp"]
    return jax.shard_map(
        functools.partial(local, ways, mp),
        mesh=mesh,
        in_specs=(
            P(None, "dp", None, None),
            P(None, None, "mp"),
            P(None, "mp", None),
            P("dp", None, None),
            P("dp", None),
            P(),
        ),
        out_specs=(P(None, "dp", "mp"), P(None, "mp", "dp"), P()),
        check_vma=False,
    )
```
